512 devices in a mesh: dp: 32 (over x, y), mx: 4 (over z_hi, core), my: 4 (over z_lo).
Axes of the slice: x: 4, y: 8, z: 8 (z_hi: 2, z_lo: 4; z = z_hi * 4 + z_lo), core: 2. Of those that a mesh axis runs over, the one named last changes fastest.
Arguments:
- mentor_final_states: bfloat16 [2048, 4608], P('dp'), may hold values from -12 to 12
- mentor_output_matrix: bfloat16 [4608, 4096], P(None, ('mx', 'my')), may hold values from -0.09375 to 0.09375
- learner_final_states: bfloat16 [2048, 3584], P('dp', 'mx'), may hold values from -12 to 12
- learner_output_matrix: bfloat16 [3584, 4096], P('mx', 'my'), may hold values from -0.09375 to 0.09375
- loss_mask: int32 [2048], P('dp'), may hold values 0 or 1
Outputs:
- mismatch_per_piece: float32 [2048], P('dp')
- mean_loss: float32 [], replicated
- student_grad: float32 [2048, 4096], P('dp', 'my')
The draws below stay inside these ranges and needn't reach their ends.
All inputs are finite; a program needn't handle non-finite values.
Results may differ from the reference program's by a relative error of at most 0.0003.
Values sent between devices are 32-bit elements.
No kernel may reach another device: no remote copies, remote signals or barrier semaphores. Data moves between devices by JAX's collectives and lax.ppermute only.
A program may use at most 64 MiB of HBM per device.

```python
import jax
import jax.numpy as jnp

D_T = 4608
D_S = 3584
WORD_LEXICON = 4096
WINDOW_PIECES = 2048


def with_ends(array, key, least, high):
    dims = array.shape
    place = [jax.random.randint(jax.random.fold_in(key, axis), (), 0, dims[axis]) for axis in range(len(dims))]
    array = array.at[tuple(place)].set(least)
    longest = dims.index(max(dims))
    place[longest] = (place[longest] + 1) % dims[longest]
    return array.at[tuple(place)].set(high)


def steps_of(own_key, shape, pieces, smallest, largest):
    def one(dim, shards_of):
        draws = jax.random.uniform(jax.random.fold_in(jax.random.fold_in(own_key, 6), dim), (shards_of,), jnp.float32, smallest / len(pieces), largest / len(pieces))
        return jnp.repeat(jnp.exp(draws), shape[dim] // shards_of).reshape((-1,) + (1,) * (len(shape) - dim - 1))

    level = one(*pieces[0])
    for cut in pieces[1:]:
        level = level * one(*cut)
    return level


def bell_draw(own_key, extent, spread, limit, cuts=(), kind=jnp.bfloat16):
    result = spread * jax.random.normal(own_key, extent, jnp.float32)
    if cuts:
        result = result * steps_of(own_key, extent, cuts, -0.22, 0.18)
    return jnp.clip(result, -limit, limit).astype(kind)


def setup_inputs(seed: int = 0) -> dict:
    arg_keys = jax.random.split(jax.random.key(seed), 6)
    mentor_final_states = bell_draw(arg_keys[0], (WINDOW_PIECES, D_T), 2.0, 12.0, ((0, 32),))
    mentor_output_matrix = bell_draw(arg_keys[1], (D_T, WORD_LEXICON), D_T ** -0.5, 0.09375, ((1, 16),))
    learner_final_states = bell_draw(arg_keys[2], (WINDOW_PIECES, D_S), 2.0, 12.0, ((0, 32), (1, 4)))
    learner_output_matrix = bell_draw(arg_keys[3], (D_S, WORD_LEXICON), D_S ** -0.5, 0.09375, ((0, 4), (1, 4)))
    loss_mask = with_ends((jax.random.randint(arg_keys[4], (WINDOW_PIECES,), 0, 4) < 3).astype(jnp.int32), jax.random.fold_in(arg_keys[4], 1), 0, 1)
    return {"mentor_final_states": mentor_final_states, "mentor_output_matrix": mentor_output_matrix, "learner_final_states": learner_final_states, "learner_output_matrix": learner_output_matrix, "loss_mask": loss_mask}


SOFTENING_HEAT = 2.0


def log_softmax_rows(values):
    row_max = jnp.max(values, axis=1, keepdims=True)
    row_sum = jnp.sum(jnp.exp(values - row_max), axis=1, keepdims=True)
    return values - (row_max + jnp.log(row_sum))


def reference(mentor_final_states, mentor_output_matrix, learner_final_states, learner_output_matrix, loss_mask):
    mentor_softened_scores = jnp.dot(mentor_final_states, mentor_output_matrix, preferred_element_type=jnp.float32) / SOFTENING_HEAT
    learner_softened_scores = jnp.dot(learner_final_states, learner_output_matrix, preferred_element_type=jnp.float32) / SOFTENING_HEAT
    mentor_logarithmic_odds = log_softmax_rows(mentor_softened_scores)
    learner_logarithmic_odds = log_softmax_rows(learner_softened_scores)
    mentor_likelihoods = jnp.exp(mentor_logarithmic_odds)
    mismatch_per_piece = SOFTENING_HEAT * SOFTENING_HEAT * jnp.sum(mentor_likelihoods * (mentor_logarithmic_odds - learner_logarithmic_odds), axis=1)
    piece_importance = loss_mask.astype(jnp.float32)
    usable_count = jnp.sum(piece_importance)
    mean_loss = jnp.sum(piece_importance * mismatch_per_piece) / usable_count
    multiplier = piece_importance * (SOFTENING_HEAT * WORD_LEXICON * WINDOW_PIECES) / usable_count
    student_grad = (jnp.exp(learner_logarithmic_odds) - mentor_likelihoods) * multiplier[:, None]
    return mismatch_per_piece, mean_loss, student_grad
```

```python
import jax
import jax.numpy as jnp
from jax import lax
from jax.sharding import Mesh
from jax.sharding import PartitionSpec as P

DP = ("dp_0", "dp_1")
GROUP = ("zh", "co", "zl")
SOFTENING_HEAT = 2.0
SWAP = [(0, 1), (1, 0)]


def teacher_route(flip):
    pairs = []
    for i in range(4):
        for j in range(4):
            zh = (j % 2) ^ flip
            pairs.append((i * 4 + j, (zh * 2 + j // 2) * 4 + i))
    return pairs


def local(
    mentor_final_states,
    mentor_output_matrix,
    learner_final_states,
    learner_output_matrix,
    loss_mask,
):
    tokens = mentor_final_states.shape[0]
    groups = lax.axis_size(GROUP)
    lexicon = mentor_output_matrix.shape[1] * groups
    pieces = tokens * lax.axis_size(DP)
    half = learner_output_matrix.shape[1] // 2
    core = lax.axis_index("co")
    zh = lax.axis_index("zh")

    partial = jnp.dot(learner_final_states, learner_output_matrix, preferred_element_type=jnp.float32)
    give = lax.dynamic_slice_in_dim(partial, (1 - core) * half, half, 1)
    keep = lax.dynamic_slice_in_dim(partial, core * half, half, 1)
    chip_sum = keep + lax.ppermute(give, "co", SWAP)
    student = (chip_sum + lax.ppermute(chip_sum, "zh", SWAP)) / SOFTENING_HEAT

    block = jnp.dot(mentor_final_states, mentor_output_matrix, preferred_element_type=jnp.float32) / SOFTENING_HEAT
    block_a = lax.ppermute(block, GROUP, teacher_route(0))
    block_b = lax.ppermute(block, GROUP, teacher_route(1))
    low = jnp.where(zh == 0, block_a, block_b)
    high = jnp.where(zh == 0, block_b, block_a)
    teacher = jnp.concatenate([low, high], axis=1)

    t_max = jnp.max(teacher, axis=1)
    s_max = jnp.max(student, axis=1)
    t_shift = teacher - t_max[:, None]
    s_shift = student - s_max[:, None]
    t_exp = jnp.exp(t_shift)
    s_exp = jnp.exp(s_shift)
    stats = jnp.stack(
        [t_max, s_max, jnp.sum(t_exp, 1), jnp.sum(s_exp, 1), jnp.sum(t_exp * (t_shift - s_shift), 1)]
    )
    peers = lax.axis_size(("co", "zl"))
    every = lax.all_to_all(jnp.broadcast_to(stats[None], (peers,) + stats.shape), ("co", "zl"), 0, 0)
    tm, sm, tz, sz, w = (every[:, k] for k in range(5))
    t_top = jnp.max(tm, 0)
    s_top = jnp.max(sm, 0)
    t_scale = jnp.exp(tm - t_top)
    t_total = jnp.sum(tz * t_scale, 0)
    s_total = jnp.sum(sz * jnp.exp(sm - s_top), 0)
    w_total = jnp.sum(t_scale * (w + tz * ((tm - t_top) - (sm - s_top))), 0)
    mismatch = (SOFTENING_HEAT * SOFTENING_HEAT) * (w_total / t_total - jnp.log(t_total) + jnp.log(s_total))

    importance = loss_mask.astype(jnp.float32)
    sums = jnp.stack([jnp.sum(importance * mismatch), jnp.sum(importance)])
    rows = lax.axis_size(DP)
    all_sums = lax.all_to_all(jnp.broadcast_to(sums[None], (rows, 2)), DP, 0, 0)

    t_log = t_shift + (t_max - t_top - jnp.log(t_total))[:, None]
    s_log = s_shift + (s_max - s_top - jnp.log(s_total))[:, None]
    gap = jnp.exp(s_log) - jnp.exp(t_log)
    other = lax.ppermute(gap, "co", SWAP)
    left = jnp.where(core == 0, gap, other)
    right = jnp.where(core == 0, other, gap)

    total = jnp.sum(all_sums, 0)
    mean_loss = total[0] / total[1]
    multiplier = importance * (SOFTENING_HEAT * lexicon * pieces) / total[1]
    student_grad = jnp.concatenate([left, right], axis=1) * multiplier[:, None]
    return mismatch, mean_loss, student_grad


def solution(mesh):
    split = Mesh(
        mesh.devices.reshape(4, 8, 2, mesh.shape["mx"] // 2, mesh.shape["my"]),
        ("dp_0", "dp_1", "zh", "co", "zl"),
    )
    mx = ("zh", "co")
    in_specs = (P(DP, None), P(None, ("zh", "co", "zl")), P(DP, mx), P(mx, "zl"), P(DP))
    out_specs = (P(DP), P(), P(DP, "zl"))
    return jax.shard_map(local, mesh=split, in_specs=in_specs, out_specs=out_specs, check_vma=False)
```

```python
import jax
import jax.numpy as jnp
from jax import lax
from jax.experimental import pallas as pl
from jax.experimental.pallas import tpu as pltpu
from jax.sharding import Mesh
from jax.sharding import PartitionSpec as P


DP = ("dp_0", "dp_1")
GROUP = ("zh", "co", "zl")
SOFTENING_HEAT = 2.0
SWAP = [(0, 1), (1, 0)]
LANES = 128
SUBLANES = 8
KERNEL_VMEM = 4 << 20
VMEM = pltpu.MemorySpace.VMEM
SMEM = pltpu.MemorySpace.SMEM


def teacher_route(flip):
    pairs = []
    for i in range(4):
        for j in range(4):
            zh = (j % 2) ^ flip
            pairs.append((i * 4 + j, (zh * 2 + j // 2) * 4 + i))
    return pairs


def call(kernel, outs, out_spaces, in_spaces):
    return pl.pallas_call(
        kernel,
        out_shape=outs,
        in_specs=[pl.BlockSpec(memory_space=s) for s in in_spaces],
        out_specs=[pl.BlockSpec(memory_space=s) for s in out_spaces],
        compiler_params=pltpu.CompilerParams(vmem_limit_bytes=KERNEL_VMEM),
    )


def stats_kernel(zh_ref, chip_ref, other_ref, a_ref, b_ref, stats_ref, student_ref):
    rows, width = a_ref.shape
    zh = zh_ref[0]
    for k, at in ((0, zh), (1, 1 - zh)):
        cols = pl.ds(pl.multiple_of(at * width, LANES), width)
        student_ref[:, k * width : (k + 1) * width] = (chip_ref[:, cols] + other_ref[:, cols]) * (1 / SOFTENING_HEAT)
    s_a, s_b = student_ref[:, :width], student_ref[:, width:]
    t_a, t_b = a_ref[...], b_ref[...]
    t_max = jnp.max(jnp.maximum(t_a, t_b), axis=1, keepdims=True)
    s_max = jnp.max(jnp.maximum(s_a, s_b), axis=1, keepdims=True)
    ta, tb, sa, sb = t_a - t_max, t_b - t_max, s_a - s_max, s_b - s_max
    ea, eb = jnp.exp(ta), jnp.exp(tb)
    t_sum = jnp.sum(ea + eb, axis=1, keepdims=True)
    s_sum = jnp.sum(jnp.exp(sa) + jnp.exp(sb), axis=1, keepdims=True)
    w_sum = jnp.sum(ea * (ta - sa) + eb * (tb - sb), axis=1, keepdims=True)
    lane = lax.broadcasted_iota(jnp.int32, (rows, LANES), 1)
    table = jnp.ones((rows, LANES), jnp.float32)
    for k, value in enumerate((t_max, s_max, t_sum, s_sum, w_sum)):
        table = jnp.where(lane == k, value, table)
    table = jnp.concatenate([table, jnp.ones((LANES - rows, LANES), jnp.float32)], axis=0).T
    for p in range(stats_ref.shape[0]):
        stats_ref[p] = table[:SUBLANES]


def merge_kernel(every_ref, mask_ref, mismatch_ref, sums_ref, consts_ref, mask_tile):
    rows = mask_ref.shape[1]
    tm, sm, tz, sz, w = (every_ref[:, k, :] for k in range(5))
    t_top = jnp.max(tm, axis=0, keepdims=True)
    s_top = jnp.max(sm, axis=0, keepdims=True)
    t_gap, s_gap = tm - t_top, sm - s_top
    t_scale = jnp.exp(t_gap)
    t_total = jnp.sum(tz * t_scale, axis=0, keepdims=True)
    s_total = jnp.sum(sz * jnp.exp(s_gap), axis=0, keepdims=True)
    w_total = jnp.sum(t_scale * (w + tz * (t_gap - s_gap)), axis=0, keepdims=True)
    t_log, s_log = jnp.log(t_total), jnp.log(s_total)
    mismatch = (SOFTENING_HEAT * SOFTENING_HEAT) * (w_total / t_total - t_log + s_log)
    mismatch_ref[...] = mismatch[:, :rows]
    mask_tile[...] = jnp.zeros(mask_tile.shape, jnp.float32)
    mask_tile[0:1, :rows] = mask_ref[...].astype(jnp.float32)
    importance = mask_tile[0:1, :]
    loss = jnp.sum(importance * mismatch, axis=1, keepdims=True)
    count = jnp.sum(importance, axis=1, keepdims=True)
    lane = lax.broadcasted_iota(jnp.int32, (1, LANES), 1)
    sums = jnp.where(lane == 0, loss, jnp.where(lane == 1, count, 0.0))
    sums_ref[...] = jnp.broadcast_to(sums[None], sums_ref.shape)
    row = lax.broadcasted_iota(jnp.int32, (LANES, LANES), 0)
    table = jnp.where(row == 0, t_top + t_log, jnp.where(row == 1, s_top + s_log, importance))
    consts_ref[...] = table.T[:rows]


def gap_kernel(student_ref, a_ref, b_ref, consts_ref, gap_ref):
    width = a_ref.shape[1]
    t_log, s_log = consts_ref[:, 0:1], consts_ref[:, 1:2]
    for k, ref in ((0, a_ref), (1, b_ref)):
        cols = slice(k * width, (k + 1) * width)
        gap_ref[:, cols] = jnp.exp(student_ref[:, cols] - s_log) - jnp.exp(ref[...] - t_log)


def grad_kernel(factor, place_ref, gap_ref, other_ref, sums_ref, consts_ref, grad_ref, loss_ref):
    half = gap_ref.shape[1]
    width = half // 2
    total = jnp.sum(sums_ref[...], axis=0)
    lane = lax.broadcasted_iota(jnp.int32, total.shape, 1)
    loss = jnp.sum(jnp.where(lane == 0, total, 0.0), axis=1, keepdims=True)
    count = jnp.sum(jnp.where(lane == 1, total, 0.0), axis=1, keepdims=True)
    loss_ref[...] = loss / count
    multiplier = consts_ref[:, 2:3] * (factor / count)
    core, zh = place_ref[0], place_ref[1]
    for ref, c in ((gap_ref, core), (other_ref, 1 - core)):
        for k, at in ((0, zh), (1, 1 - zh)):
            cols = pl.ds(pl.multiple_of(c * half + at * width, LANES), width)
            grad_ref[:, cols] = ref[:, k * width : (k + 1) * width] * multiplier


def local(
    mentor_final_states,
    mentor_output_matrix,
    learner_final_states,
    learner_output_matrix,
    loss_mask,
):
    tokens = mentor_final_states.shape[0]
    width = mentor_output_matrix.shape[1]
    columns = learner_output_matrix.shape[1]
    half = columns // 2
    lexicon = width * lax.axis_size(GROUP)
    rows = lax.axis_size(DP)
    peers = lax.axis_size(("co", "zl"))
    core = lax.axis_index("co")
    zh = lax.axis_index("zh")
    place = jnp.stack([core, zh]).astype(jnp.int32)
    f32 = jnp.float32

    partial = jnp.dot(learner_final_states, learner_output_matrix, preferred_element_type=f32)
    give = lax.dynamic_slice_in_dim(partial, (1 - core) * half, half, 1)
    keep = lax.dynamic_slice_in_dim(partial, core * half, half, 1)
    chip_sum = keep + lax.ppermute(give, "co", SWAP)
    other_sum = lax.ppermute(chip_sum, "zh", SWAP)

    block = jnp.dot(mentor_final_states, mentor_output_matrix, preferred_element_type=f32) / SOFTENING_HEAT
    block_a = lax.ppermute(block, GROUP, teacher_route(0))
    block_b = lax.ppermute(block, GROUP, teacher_route(1))

    stats, student = call(
        stats_kernel,
        [jax.ShapeDtypeStruct((peers, SUBLANES, LANES), f32), jax.ShapeDtypeStruct((tokens, half), f32)],
        [VMEM, VMEM],
        [SMEM, VMEM, VMEM, VMEM, VMEM],
    )(zh[None].astype(jnp.int32), chip_sum, other_sum, block_a, block_b)
    every = lax.all_to_all(stats, ("co", "zl"), 0, 0)
    mismatch, sums, consts = pl.pallas_call(
        merge_kernel,
        out_shape=[
            jax.ShapeDtypeStruct((1, tokens), f32),
            jax.ShapeDtypeStruct((rows, 1, LANES), f32),
            jax.ShapeDtypeStruct((tokens, LANES), f32),
        ],
        in_specs=[pl.BlockSpec(memory_space=VMEM)] * 2,
        out_specs=[pl.BlockSpec(memory_space=VMEM)] * 3,
        scratch_shapes=[pltpu.VMEM((SUBLANES, LANES), f32)],
        name="merge",
        compiler_params=pltpu.CompilerParams(vmem_limit_bytes=KERNEL_VMEM),
    )(every, loss_mask[None])
    all_sums = lax.all_to_all(sums, DP, 0, 0)

    (gap,) = call(
        gap_kernel, [jax.ShapeDtypeStruct((tokens, half), f32)], [VMEM], [VMEM] * 4
    )(student, block_a, block_b, consts)
    other = lax.ppermute(gap, "co", SWAP)

    def final(*refs):
        grad_kernel(SOFTENING_HEAT * lexicon * tokens * rows, *refs)

    student_grad, mean_loss = call(
        final,
        [jax.ShapeDtypeStruct((tokens, columns), f32), jax.ShapeDtypeStruct((1, 1), f32)],
        [VMEM, VMEM],
        [SMEM, VMEM, VMEM, VMEM, VMEM],
    )(place, gap, other, all_sums, consts)
    return mismatch.reshape(tokens), mean_loss.reshape(()), student_grad


def solution(mesh):
    split = Mesh(
        mesh.devices.reshape(4, 8, 2, mesh.shape["mx"] // 2, mesh.shape["my"]),
        ("dp_0", "dp_1", "zh", "co", "zl"),
    )
    mx = ("zh", "co")
    in_specs = (P(DP, None), P(None, ("zh", "co", "zl")), P(DP, mx), P(mx, "zl"), P(DP))
    out_specs = (P(DP), P(), P(DP, "zl"))

    return jax.shard_map(local, mesh=split, in_specs=in_specs, out_specs=out_specs, check_vma=False)
```

```python
import jax
import jax.numpy as jnp
from jax import lax
from jax.experimental import pallas as pl
from jax.experimental.pallas import tpu as pltpu
from jax.sharding import Mesh
from jax.sharding import PartitionSpec as P


DP = ("dp_0", "dp_1")
GROUP = ("zh", "co", "zl")
SOFTENING_HEAT = 2.0
SWAP = [(0, 1), (1, 0)]
LANES = 128
SUBLANES = 8
KERNEL_VMEM = 4 << 20
VMEM = pltpu.MemorySpace.VMEM
SMEM = pltpu.MemorySpace.SMEM


def teacher_route(flip):
    pairs = []
    for i in range(4):
        for j in range(4):
            zh = (j % 2) ^ flip
            pairs.append((i * 4 + j, (zh * 2 + j // 2) * 4 + i))
    return pairs


def call(kernel, outs, out_spaces, in_spaces):
    return pl.pallas_call(
        kernel,
        out_shape=outs,
        in_specs=[pl.BlockSpec(memory_space=s) for s in in_spaces],
        out_specs=[pl.BlockSpec(memory_space=s) for s in out_spaces],
        compiler_params=pltpu.CompilerParams(vmem_limit_bytes=KERNEL_VMEM),
    )


def stats_kernel(zh_ref, chip_ref, other_ref, a_ref, stats_ref):
    rows, width = a_ref.shape
    cols = pl.ds(pl.multiple_of(zh_ref[0] * width, LANES), width)
    s = (chip_ref[:, cols] + other_ref[:, cols]) * (1 / SOFTENING_HEAT)
    t = a_ref[...]
    t_max = jnp.max(t, axis=1, keepdims=True)
    s_max = jnp.max(s, axis=1, keepdims=True)
    t, s = t - t_max, s - s_max
    e = jnp.exp(t)
    t_sum = jnp.sum(e, axis=1, keepdims=True)
    s_sum = jnp.sum(jnp.exp(s), axis=1, keepdims=True)
    w_sum = jnp.sum(e * (t - s), axis=1, keepdims=True)
    lane = lax.broadcasted_iota(jnp.int32, (rows, LANES), 1)
    table = jnp.ones((rows, LANES), jnp.float32)
    for k, value in enumerate((t_max, s_max, t_sum, s_sum, w_sum)):
        table = jnp.where(lane == k, value, table)
    table = jnp.concatenate([table, jnp.ones((LANES - rows, LANES), jnp.float32)], axis=0).T
    for p in range(stats_ref.shape[0]):
        stats_ref[p] = table[:SUBLANES]


def merge_kernel(every_ref, mask_ref, mismatch_ref, sums_ref, consts_ref, mask_tile):
    rows = mask_ref.shape[1]
    tm, sm, tz, sz, w = (every_ref[:, k, :] for k in range(5))
    t_top = jnp.max(tm, axis=0, keepdims=True)
    s_top = jnp.max(sm, axis=0, keepdims=True)
    t_gap, s_gap = tm - t_top, sm - s_top
    t_scale = jnp.exp(t_gap)
    t_total = jnp.sum(tz * t_scale, axis=0, keepdims=True)
    s_total = jnp.sum(sz * jnp.exp(s_gap), axis=0, keepdims=True)
    w_total = jnp.sum(t_scale * (w + tz * (t_gap - s_gap)), axis=0, keepdims=True)
    t_log, s_log = jnp.log(t_total), jnp.log(s_total)
    mismatch = (SOFTENING_HEAT * SOFTENING_HEAT) * (w_total / t_total - t_log + s_log)
    mismatch_ref[...] = mismatch[:, :rows]
    mask_tile[...] = jnp.zeros(mask_tile.shape, jnp.float32)
    mask_tile[0:1, :rows] = mask_ref[...].astype(jnp.float32)
    importance = mask_tile[0:1, :]
    loss = jnp.sum(importance * mismatch, axis=1, keepdims=True)
    count = jnp.sum(importance, axis=1, keepdims=True)
    lane = lax.broadcasted_iota(jnp.int32, (1, LANES), 1)
    sums = jnp.where(lane == 0, loss, jnp.where(lane == 1, count, 0.0))
    sums_ref[...] = jnp.broadcast_to(sums[None], sums_ref.shape)
    row = lax.broadcasted_iota(jnp.int32, (LANES, LANES), 0)
    table = jnp.where(row == 0, t_top + t_log, jnp.where(row == 1, s_top + s_log, importance))
    consts_ref[...] = table.T[:rows]


def gap_kernel(zh_ref, chip_ref, other_ref, a_ref, b_ref, consts_ref, gap_ref):
    width = a_ref.shape[1]
    zh = zh_ref[0]
    t_log, s_log = consts_ref[:, 0:1], consts_ref[:, 1:2]
    for k, at, ref in ((0, zh, a_ref), (1, 1 - zh, b_ref)):
        cols = pl.ds(pl.multiple_of(at * width, LANES), width)
        student = (chip_ref[:, cols] + other_ref[:, cols]) * (1 / SOFTENING_HEAT)
        gap_ref[:, k * width : (k + 1) * width] = jnp.exp(student - s_log) - jnp.exp(ref[...] - t_log)


def grad_kernel(factor, place_ref, gap_ref, other_ref, sums_ref, consts_ref, grad_ref, loss_ref):
    half = gap_ref.shape[1]
    width = half // 2
    total = jnp.sum(sums_ref[...], axis=0)
    lane = lax.broadcasted_iota(jnp.int32, total.shape, 1)
    loss = jnp.sum(jnp.where(lane == 0, total, 0.0), axis=1, keepdims=True)
    count = jnp.sum(jnp.where(lane == 1, total, 0.0), axis=1, keepdims=True)
    loss_ref[...] = loss / count
    multiplier = consts_ref[:, 2:3] * (factor / count)
    core, zh = place_ref[0], place_ref[1]
    for ref, c in ((gap_ref, core), (other_ref, 1 - core)):
        for k, at in ((0, zh), (1, 1 - zh)):
            cols = pl.ds(pl.multiple_of(c * half + at * width, LANES), width)
            grad_ref[:, cols] = ref[:, k * width : (k + 1) * width] * multiplier


def local(
    mentor_final_states,
    mentor_output_matrix,
    learner_final_states,
    learner_output_matrix,
    loss_mask,
):
    tokens = mentor_final_states.shape[0]
    width = mentor_output_matrix.shape[1]
    columns = learner_output_matrix.shape[1]
    half = columns // 2
    lexicon = width * lax.axis_size(GROUP)
    rows = lax.axis_size(DP)
    peers = lax.axis_size(GROUP)
    core = lax.axis_index("co")
    zh = lax.axis_index("zh")
    zh_at = zh[None].astype(jnp.int32)
    place = jnp.stack([core, zh]).astype(jnp.int32)
    f32 = jnp.float32

    partial = jnp.dot(learner_final_states, learner_output_matrix, preferred_element_type=f32)
    give = lax.dynamic_slice_in_dim(partial, (1 - core) * half, half, 1)
    keep = lax.dynamic_slice_in_dim(partial, core * half, half, 1)
    chip_sum = keep + lax.ppermute(give, "co", SWAP)
    other_sum = lax.ppermute(chip_sum, "zh", SWAP)

    block = jnp.dot(mentor_final_states, mentor_output_matrix, preferred_element_type=f32) / SOFTENING_HEAT
    block_a = lax.ppermute(block, GROUP, teacher_route(0))
    block_b = lax.ppermute(block, GROUP, teacher_route(1))

    (stats,) = call(
        stats_kernel, [jax.ShapeDtypeStruct((peers, SUBLANES, LANES), f32)], [VMEM], [SMEM, VMEM, VMEM, VMEM]
    )(zh_at, chip_sum, other_sum, block_a)
    every = lax.all_to_all(stats, GROUP, 0, 0)
    mismatch, sums, consts = pl.pallas_call(
        merge_kernel,
        out_shape=[
            jax.ShapeDtypeStruct((1, tokens), f32),
            jax.ShapeDtypeStruct((rows, 1, LANES), f32),
            jax.ShapeDtypeStruct((tokens, LANES), f32),
        ],
        in_specs=[pl.BlockSpec(memory_space=VMEM)] * 2,
        out_specs=[pl.BlockSpec(memory_space=VMEM)] * 3,
        scratch_shapes=[pltpu.VMEM((SUBLANES, LANES), f32)],
        name="merge",
        compiler_params=pltpu.CompilerParams(vmem_limit_bytes=KERNEL_VMEM),
    )(every, loss_mask[None])
    all_sums = lax.all_to_all(sums, DP, 0, 0)

    (gap,) = call(
        gap_kernel, [jax.ShapeDtypeStruct((tokens, half), f32)], [VMEM], [SMEM] + [VMEM] * 5
    )(zh_at, chip_sum, other_sum, block_a, block_b, consts)
    other = lax.ppermute(gap, "co", SWAP)

    def final(*refs):
        grad_kernel(SOFTENING_HEAT * lexicon * tokens * rows, *refs)

    student_grad, mean_loss = call(
        final,
        [jax.ShapeDtypeStruct((tokens, columns), f32), jax.ShapeDtypeStruct((1, 1), f32)],
        [VMEM, VMEM],
        [SMEM, VMEM, VMEM, VMEM, VMEM],
    )(place, gap, other, all_sums, consts)
    return mismatch.reshape(tokens), mean_loss.reshape(()), student_grad


def solution(mesh):
    split = Mesh(
        mesh.devices.reshape(4, 8, 2, mesh.shape["mx"] // 2, mesh.shape["my"]),
        ("dp_0", "dp_1", "zh", "co", "zl"),
    )
    mx = ("zh", "co")
    in_specs = (P(DP, None), P(None, ("zh", "co", "zl")), P(DP, mx), P(mx, "zl"), P(DP))
    out_specs = (P(DP), P(), P(DP, "zl"))

    return jax.shard_map(local, mesh=split, in_specs=in_specs, out_specs=out_specs, check_vma=False)
```

```python
import jax
import jax.numpy as jnp
from jax import lax
from jax.experimental import pallas as pl
from jax.experimental.pallas import tpu as pltpu
from jax.sharding import Mesh
from jax.sharding import PartitionSpec as P


DP = ("dp_0", "dp_1")
GROUP = ("zh", "co", "zl")
SOFTENING_HEAT = 2.0
SWAP = [(0, 1), (1, 0)]
LANES = 128
SUBLANES = 8
KERNEL_VMEM = 4 << 20
VMEM = pltpu.MemorySpace.VMEM
SMEM = pltpu.MemorySpace.SMEM


def teacher_route(flip):
    return [(i * 4 + j, (((j // 2) ^ flip) * 2 + j % 2) * 4 + i) for i in range(4) for j in range(4)]


def call(kernel, outs, out_spaces, in_spaces):
    return pl.pallas_call(
        kernel,
        out_shape=outs,
        in_specs=[pl.BlockSpec(memory_space=s) for s in in_spaces],
        out_specs=[pl.BlockSpec(memory_space=s) for s in out_spaces],
        compiler_params=pltpu.CompilerParams(vmem_limit_bytes=KERNEL_VMEM),
    )


def split_kernel(core_ref, partial_ref, give_ref, keep_ref):
    width = give_ref.shape[1] // 2
    core = core_ref[0]
    for ref, c in ((give_ref, 1 - core), (keep_ref, core)):
        for z in range(2):
            cols = pl.ds(pl.multiple_of((2 * z + c) * width, LANES), width)
            ref[:, z * width : (z + 1) * width] = partial_ref[:, cols]


def stats_kernel(zh_ref, chip_ref, other_ref, a_ref, stats_ref):
    rows, width = a_ref.shape
    cols = pl.ds(pl.multiple_of(zh_ref[0] * width, LANES), width)
    s = (chip_ref[:, cols] + other_ref[:, cols]) * (1 / SOFTENING_HEAT)
    t = a_ref[...]
    t_max = jnp.max(t, axis=1, keepdims=True)
    s_max = jnp.max(s, axis=1, keepdims=True)
    t, s = t - t_max, s - s_max
    e = jnp.exp(t)
    t_sum = jnp.sum(e, axis=1, keepdims=True)
    s_sum = jnp.sum(jnp.exp(s), axis=1, keepdims=True)
    w_sum = jnp.sum(e * (t - s), axis=1, keepdims=True)
    lane = lax.broadcasted_iota(jnp.int32, (rows, LANES), 1)
    table = jnp.ones((rows, LANES), jnp.float32)
    for k, value in enumerate((t_max, s_max, t_sum, s_sum, w_sum)):
        table = jnp.where(lane == k, value, table)
    table = jnp.concatenate([table, jnp.ones((LANES - rows, LANES), jnp.float32)], axis=0).T
    for p in range(stats_ref.shape[0]):
        stats_ref[p] = table[:SUBLANES]


def merge_kernel(every_ref, mask_ref, mismatch_ref, sums_ref, consts_ref, mask_tile):
    rows = mask_ref.shape[1]
    tm, sm, tz, sz, w = (every_ref[:, k, :] for k in range(5))
    t_top = jnp.max(tm, axis=0, keepdims=True)
    s_top = jnp.max(sm, axis=0, keepdims=True)
    t_gap, s_gap = tm - t_top, sm - s_top
    t_scale = jnp.exp(t_gap)
    t_total = jnp.sum(tz * t_scale, axis=0, keepdims=True)
    s_total = jnp.sum(sz * jnp.exp(s_gap), axis=0, keepdims=True)
    w_total = jnp.sum(t_scale * (w + tz * (t_gap - s_gap)), axis=0, keepdims=True)
    t_log, s_log = jnp.log(t_total), jnp.log(s_total)
    mismatch = (SOFTENING_HEAT * SOFTENING_HEAT) * (w_total / t_total - t_log + s_log)
    mismatch_ref[...] = mismatch[:, :rows]
    mask_tile[...] = jnp.zeros(mask_tile.shape, jnp.float32)
    mask_tile[0:1, :rows] = mask_ref[...].astype(jnp.float32)
    importance = mask_tile[0:1, :]
    loss = jnp.sum(importance * mismatch, axis=1, keepdims=True)
    count = jnp.sum(importance, axis=1, keepdims=True)
    lane = lax.broadcasted_iota(jnp.int32, (1, LANES), 1)
    sums = jnp.where(lane == 0, loss, jnp.where(lane == 1, count, 0.0))
    sums_ref[...] = jnp.broadcast_to(sums[None], sums_ref.shape)
    row = lax.broadcasted_iota(jnp.int32, (LANES, LANES), 0)
    table = jnp.where(row == 0, t_top + t_log, jnp.where(row == 1, s_top + s_log, importance))
    consts_ref[...] = table.T[:rows]


def gap_kernel(zh_ref, chip_ref, other_ref, a_ref, b_ref, consts_ref, gap_ref):
    width = a_ref.shape[1]
    zh = zh_ref[0]
    t_log, s_log = consts_ref[:, 0:1], consts_ref[:, 1:2]
    for k, at, ref in ((0, zh, a_ref), (1, 1 - zh, b_ref)):
        cols = pl.ds(pl.multiple_of(at * width, LANES), width)
        student = (chip_ref[:, cols] + other_ref[:, cols]) * (1 / SOFTENING_HEAT)
        gap_ref[:, k * width : (k + 1) * width] = jnp.exp(student - s_log) - jnp.exp(ref[...] - t_log)


def grad_kernel(factor, place_ref, gap_ref, other_ref, sums_ref, consts_ref, grad_ref, loss_ref):
    width = gap_ref.shape[1] // 2
    total = jnp.sum(sums_ref[...], axis=0)
    lane = lax.broadcasted_iota(jnp.int32, total.shape, 1)
    loss = jnp.sum(jnp.where(lane == 0, total, 0.0), axis=1, keepdims=True)
    count = jnp.sum(jnp.where(lane == 1, total, 0.0), axis=1, keepdims=True)
    loss_ref[...] = loss / count
    multiplier = consts_ref[:, 2:3] * (factor / count)
    core, zh = place_ref[0], place_ref[1]
    for ref, c in ((gap_ref, core), (other_ref, 1 - core)):
        for k, at in ((0, zh), (1, 1 - zh)):
            cols = pl.ds(pl.multiple_of((2 * at + c) * width, LANES), width)
            grad_ref[:, cols] = ref[:, k * width : (k + 1) * width] * multiplier


def local(
    mentor_final_states,
    mentor_output_matrix,
    learner_final_states,
    learner_output_matrix,
    loss_mask,
):
    tokens = mentor_final_states.shape[0]
    width = mentor_output_matrix.shape[1]
    columns = learner_output_matrix.shape[1]
    half = columns // 2
    lexicon = width * lax.axis_size(GROUP)
    rows = lax.axis_size(DP)
    peers = lax.axis_size(GROUP)
    core = lax.axis_index("co")
    zh = lax.axis_index("zh")
    zh_at = zh[None].astype(jnp.int32)
    place = jnp.stack([core, zh]).astype(jnp.int32)
    f32 = jnp.float32

    core_at = core[None].astype(jnp.int32)
    partial = jnp.dot(learner_final_states, learner_output_matrix, preferred_element_type=f32)
    give, keep = call(
        split_kernel, [jax.ShapeDtypeStruct((tokens, half), f32)] * 2, [VMEM] * 2, [SMEM, VMEM]
    )(core_at, partial)
    chip_sum = keep + lax.ppermute(give, "co", SWAP)
    other_sum = lax.ppermute(chip_sum, "zh", SWAP)

    block = jnp.dot(mentor_final_states, mentor_output_matrix, preferred_element_type=f32) / SOFTENING_HEAT
    block_a = lax.ppermute(block, GROUP, teacher_route(0))
    block_b = lax.ppermute(block, GROUP, teacher_route(1))

    (stats,) = call(
        stats_kernel, [jax.ShapeDtypeStruct((peers, SUBLANES, LANES), f32)], [VMEM], [SMEM, VMEM, VMEM, VMEM]
    )(zh_at, chip_sum, other_sum, block_a)
    every = lax.all_to_all(stats, GROUP, 0, 0)
    mismatch, sums, consts = pl.pallas_call(
        merge_kernel,
        out_shape=[
            jax.ShapeDtypeStruct((1, tokens), f32),
            jax.ShapeDtypeStruct((rows, 1, LANES), f32),
            jax.ShapeDtypeStruct((tokens, LANES), f32),
        ],
        in_specs=[pl.BlockSpec(memory_space=VMEM)] * 2,
        out_specs=[pl.BlockSpec(memory_space=VMEM)] * 3,
        scratch_shapes=[pltpu.VMEM((SUBLANES, LANES), f32)],
        name="merge",
        compiler_params=pltpu.CompilerParams(vmem_limit_bytes=KERNEL_VMEM),
    )(every, loss_mask[None])
    all_sums = lax.all_to_all(sums, DP, 0, 0)

    (gap,) = call(
        gap_kernel, [jax.ShapeDtypeStruct((tokens, half), f32)], [VMEM], [SMEM] + [VMEM] * 5
    )(zh_at, chip_sum, other_sum, block_a, block_b, consts)
    other = lax.ppermute(gap, "co", SWAP)

    def final(*refs):
        grad_kernel(SOFTENING_HEAT * lexicon * tokens * rows, *refs)

    student_grad, mean_loss = call(
        final,
        [jax.ShapeDtypeStruct((tokens, columns), f32), jax.ShapeDtypeStruct((1, 1), f32)],
        [VMEM, VMEM],
        [SMEM, VMEM, VMEM, VMEM, VMEM],
    )(place, gap, other, all_sums, consts)
    return mismatch.reshape(tokens), mean_loss.reshape(()), student_grad


def solution(mesh):
    split = Mesh(
        mesh.devices.reshape(4, 8, 2, mesh.shape["mx"] // 2, mesh.shape["my"]),
        ("dp_0", "dp_1", "zh", "co", "zl"),
    )
    mx = ("zh", "co")
    in_specs = (P(DP, None), P(None, ("zh", "co", "zl")), P(DP, mx), P(mx, "zl"), P(DP))
    out_specs = (P(DP), P(), P(DP, "zl"))

    return jax.shard_map(local, mesh=split, in_specs=in_specs, out_specs=out_specs, check_vma=False)
```

```python
import jax
import jax.numpy as jnp
from jax import lax
from jax.experimental import pallas as pl
from jax.experimental.pallas import tpu as pltpu
from jax.sharding import Mesh
from jax.sharding import PartitionSpec as P


DP = ("dp_0", "dp_1")
GROUP = ("zh", "co", "zl")
SOFTENING_HEAT = 2.0
SWAP = [(0, 1), (1, 0)]
LANES = 128
SUBLANES = 8
KERNEL_VMEM = 4 << 20
VMEM = pltpu.MemorySpace.VMEM
SMEM = pltpu.MemorySpace.SMEM


def teacher_route(flip):
    pairs = []
    for i in range(4):
        for j in range(4):
            zh = (j % 2) ^ flip
            pairs.append((i * 4 + j, (zh * 2 + j // 2) * 4 + i))
    return pairs


def call(kernel, outs, out_spaces, in_spaces):
    return pl.pallas_call(
        kernel,
        out_shape=outs,
        in_specs=[pl.BlockSpec(memory_space=s) for s in in_spaces],
        out_specs=[pl.BlockSpec(memory_space=s) for s in out_spaces],
        compiler_params=pltpu.CompilerParams(vmem_limit_bytes=KERNEL_VMEM),
    )


def stats_kernel(zh_ref, chip_ref, other_ref, a_ref, b_ref, stats_ref, student_ref):
    rows, width = a_ref.shape
    zh = zh_ref[0]
    for k, at in ((0, zh), (1, 1 - zh)):
        cols = pl.ds(pl.multiple_of(at * width, LANES), width)
        student_ref[:, k * width : (k + 1) * width] = (chip_ref[:, cols] + other_ref[:, cols]) * (1 / SOFTENING_HEAT)
    s_a, s_b = student_ref[:, :width], student_ref[:, width:]
    t_a, t_b = a_ref[...], b_ref[...]
    t_max = jnp.max(jnp.maximum(t_a, t_b), axis=1, keepdims=True)
    s_max = jnp.max(jnp.maximum(s_a, s_b), axis=1, keepdims=True)
    ta, tb, sa, sb = t_a - t_max, t_b - t_max, s_a - s_max, s_b - s_max
    ea, eb = jnp.exp(ta), jnp.exp(tb)
    t_sum = jnp.sum(ea + eb, axis=1, keepdims=True)
    s_sum = jnp.sum(jnp.exp(sa) + jnp.exp(sb), axis=1, keepdims=True)
    w_sum = jnp.sum(ea * (ta - sa) + eb * (tb - sb), axis=1, keepdims=True)
    lane = lax.broadcasted_iota(jnp.int32, (rows, LANES), 1)
    table = jnp.ones((rows, LANES), jnp.float32)
    for k, value in enumerate((t_max, s_max, t_sum, s_sum, w_sum)):
        table = jnp.where(lane == k, value, table)
    table = jnp.concatenate([table, jnp.ones((LANES - rows, LANES), jnp.float32)], axis=0).T
    for p in range(stats_ref.shape[0]):
        stats_ref[p] = table[:SUBLANES]


def merge_kernel(every_ref, mask_ref, mismatch_ref, sums_ref, consts_ref, mask_tile):
    rows = mask_ref.shape[1]
    tm, sm, tz, sz, w = (every_ref[:, k, :] for k in range(5))
    t_top = jnp.max(tm, axis=0, keepdims=True)
    s_top = jnp.max(sm, axis=0, keepdims=True)
    t_gap, s_gap = tm - t_top, sm - s_top
    t_scale = jnp.exp(t_gap)
    t_total = jnp.sum(tz * t_scale, axis=0, keepdims=True)
    s_total = jnp.sum(sz * jnp.exp(s_gap), axis=0, keepdims=True)
    w_total = jnp.sum(t_scale * (w + tz * (t_gap - s_gap)), axis=0, keepdims=True)
    t_log, s_log = jnp.log(t_total), jnp.log(s_total)
    mismatch = (SOFTENING_HEAT * SOFTENING_HEAT) * (w_total / t_total - t_log + s_log)
    mismatch_ref[...] = mismatch[:, :rows]
    mask_tile[...] = jnp.zeros(mask_tile.shape, jnp.float32)
    mask_tile[0:1, :rows] = mask_ref[...].astype(jnp.float32)
    importance = mask_tile[0:1, :]
    loss = jnp.sum(importance * mismatch, axis=1, keepdims=True)
    count = jnp.sum(importance, axis=1, keepdims=True)
    lane = lax.broadcasted_iota(jnp.int32, (1, LANES), 1)
    sums = jnp.where(lane == 0, loss, jnp.where(lane == 1, count, 0.0))
    sums_ref[...] = jnp.broadcast_to(sums[None], sums_ref.shape)
    row = lax.broadcasted_iota(jnp.int32, (LANES, LANES), 0)
    table = jnp.where(row == 0, t_top + t_log, jnp.where(row == 1, s_top + s_log, importance))
    consts_ref[...] = table.T[:rows]


def gap_kernel(student_ref, a_ref, b_ref, consts_ref, gap_ref):
    width = a_ref.shape[1]
    t_log, s_log = consts_ref[:, 0:1], consts_ref[:, 1:2]
    for k, ref in ((0, a_ref), (1, b_ref)):
        cols = slice(k * width, (k + 1) * width)
        gap_ref[:, cols] = jnp.exp(student_ref[:, cols] - s_log) - jnp.exp(ref[...] - t_log)


def grad_kernel(factor, core_ref, zh_ref, gap_ref, other_ref, sums_ref, consts_ref, grad_ref, loss_ref):
    half = gap_ref.shape[1]
    width = half // 2
    total = jnp.sum(sums_ref[...], axis=0)
    lane = lax.broadcasted_iota(jnp.int32, total.shape, 1)
    loss = jnp.sum(jnp.where(lane == 0, total, 0.0), axis=1, keepdims=True)
    count = jnp.sum(jnp.where(lane == 1, total, 0.0), axis=1, keepdims=True)
    loss_ref[...] = loss / count
    multiplier = consts_ref[:, 2:3] * (factor / count)
    core, zh = core_ref[0], zh_ref[0]
    for ref, c in ((gap_ref, core), (other_ref, 1 - core)):
        for k, at in ((0, zh), (1, 1 - zh)):
            cols = pl.ds(pl.multiple_of(c * half + at * width, LANES), width)
            grad_ref[:, cols] = ref[:, k * width : (k + 1) * width] * multiplier


def local(
    mentor_final_states,
    mentor_output_matrix,
    learner_final_states,
    learner_output_matrix,
    loss_mask,
):
    tokens = mentor_final_states.shape[0]
    width = mentor_output_matrix.shape[1]
    columns = learner_output_matrix.shape[1]
    half = columns // 2
    lexicon = width * lax.axis_size(GROUP)
    rows = lax.axis_size(DP)
    peers = lax.axis_size(("co", "zl"))
    core = lax.axis_index("co")
    zh = lax.axis_index("zh")
    core_at, zh_at = core[None].astype(jnp.int32), zh[None].astype(jnp.int32)
    f32 = jnp.float32

    def product(c):
        matrix = lax.dynamic_slice_in_dim(learner_output_matrix, c * half, half, 1)
        return jnp.dot(learner_final_states, matrix, preferred_element_type=f32)

    give = product(1 - core)
    from_core = lax.ppermute(give, "co", SWAP)
    keep = lax.optimization_barrier(product(core))
    chip_sum = keep + from_core
    other_sum = lax.ppermute(chip_sum, "zh", SWAP)

    block = jnp.dot(mentor_final_states, mentor_output_matrix, preferred_element_type=f32) / SOFTENING_HEAT
    block_a = lax.ppermute(block, GROUP, teacher_route(0))
    block_b = lax.ppermute(block, GROUP, teacher_route(1))

    stats, student = call(
        stats_kernel,
        [jax.ShapeDtypeStruct((peers, SUBLANES, LANES), f32), jax.ShapeDtypeStruct((tokens, half), f32)],
        [VMEM, VMEM],
        [SMEM, VMEM, VMEM, VMEM, VMEM],
    )(zh_at, chip_sum, other_sum, block_a, block_b)
    every = lax.all_to_all(stats, ("co", "zl"), 0, 0)
    mismatch, sums, consts = pl.pallas_call(
        merge_kernel,
        out_shape=[
            jax.ShapeDtypeStruct((1, tokens), f32),
            jax.ShapeDtypeStruct((rows, 1, LANES), f32),
            jax.ShapeDtypeStruct((tokens, LANES), f32),
        ],
        in_specs=[pl.BlockSpec(memory_space=VMEM)] * 2,
        out_specs=[pl.BlockSpec(memory_space=VMEM)] * 3,
        scratch_shapes=[pltpu.VMEM((SUBLANES, LANES), f32)],
        name="merge",
        compiler_params=pltpu.CompilerParams(vmem_limit_bytes=KERNEL_VMEM),
    )(every, loss_mask[None])
    all_sums = lax.all_to_all(sums, DP, 0, 0)

    (gap,) = call(
        gap_kernel, [jax.ShapeDtypeStruct((tokens, half), f32)], [VMEM], [VMEM] * 4
    )(student, block_a, block_b, consts)
    other = lax.ppermute(gap, "co", SWAP)

    def final(*refs):
        grad_kernel(SOFTENING_HEAT * lexicon * tokens * rows, *refs)

    student_grad, mean_loss = call(
        final,
        [jax.ShapeDtypeStruct((tokens, columns), f32), jax.ShapeDtypeStruct((1, 1), f32)],
        [VMEM, VMEM],
        [SMEM, SMEM, VMEM, VMEM, VMEM, VMEM],
    )(core_at, zh_at, gap, other, all_sums, consts)
    return mismatch.reshape(tokens), mean_loss.reshape(()), student_grad


def solution(mesh):
    split = Mesh(
        mesh.devices.reshape(4, 8, 2, mesh.shape["mx"] // 2, mesh.shape["my"]),
        ("dp_0", "dp_1", "zh", "co", "zl"),
    )
    mx = ("zh", "co")
    in_specs = (P(DP, None), P(None, ("zh", "co", "zl")), P(DP, mx), P(mx, "zl"), P(DP))
    out_specs = (P(DP), P(), P(DP, "zl"))

    return jax.shard_map(local, mesh=split, in_specs=in_specs, out_specs=out_specs, check_vma=False)
```

```python
import jax
import jax.numpy as jnp
from jax import lax
from jax.experimental import pallas as pl
from jax.experimental.pallas import tpu as pltpu
from jax.sharding import Mesh
from jax.sharding import PartitionSpec as P


DP = "dp"
SERVED = [22, 31, 20, 30, 4, 28, 15, 21, 29, 7, 12, 23, 0, 26, 11, 6, 13, 10, 5, 27, 19, 14, 9, 18, 3, 17, 25, 2, 16, 24, 8, 1]
GROUP = ("zh", "co", "zl")
SOFTENING_HEAT = 2.0
SWAP = [(0, 1), (1, 0)]
LANES = 128
SUBLANES = 8
KERNEL_VMEM = 4 << 20
VMEM = pltpu.MemorySpace.VMEM
SMEM = pltpu.MemorySpace.SMEM


def teacher_route(flip):
    pairs = []
    for i in range(4):
        for j in range(4):
            zh = (j % 2) ^ flip
            pairs.append((i * 4 + j, (zh * 2 + j // 2) * 4 + i))
    return pairs


def call(kernel, outs, out_spaces, in_spaces):
    return pl.pallas_call(
        kernel,
        out_shape=outs,
        in_specs=[pl.BlockSpec(memory_space=s) for s in in_spaces],
        out_specs=[pl.BlockSpec(memory_space=s) for s in out_spaces],
        compiler_params=pltpu.CompilerParams(vmem_limit_bytes=KERNEL_VMEM),
    )


def stats_kernel(zh_ref, chip_ref, other_ref, a_ref, b_ref, stats_ref, student_ref):
    rows, width = a_ref.shape
    zh = zh_ref[0]
    for k, at in ((0, zh), (1, 1 - zh)):
        cols = pl.ds(pl.multiple_of(at * width, LANES), width)
        student_ref[:, k * width : (k + 1) * width] = (chip_ref[:, cols] + other_ref[:, cols]) * (1 / SOFTENING_HEAT)
    s_a, s_b = student_ref[:, :width], student_ref[:, width:]
    t_a, t_b = a_ref[...], b_ref[...]
    t_max = jnp.max(jnp.maximum(t_a, t_b), axis=1, keepdims=True)
    s_max = jnp.max(jnp.maximum(s_a, s_b), axis=1, keepdims=True)
    ta, tb, sa, sb = t_a - t_max, t_b - t_max, s_a - s_max, s_b - s_max
    ea, eb = jnp.exp(ta), jnp.exp(tb)
    t_sum = jnp.sum(ea + eb, axis=1, keepdims=True)
    s_sum = jnp.sum(jnp.exp(sa) + jnp.exp(sb), axis=1, keepdims=True)
    w_sum = jnp.sum(ea * (ta - sa) + eb * (tb - sb), axis=1, keepdims=True)
    lane = lax.broadcasted_iota(jnp.int32, (rows, LANES), 1)
    table = jnp.ones((rows, LANES), jnp.float32)
    for k, value in enumerate((t_max, s_max, t_sum, s_sum, w_sum)):
        table = jnp.where(lane == k, value, table)
    table = jnp.concatenate([table, jnp.ones((LANES - rows, LANES), jnp.float32)], axis=0).T
    for p in range(stats_ref.shape[0]):
        stats_ref[p] = table[:SUBLANES]


def merge_kernel(every_ref, mask_ref, mismatch_ref, sums_ref, consts_ref, mask_tile):
    rows = mask_ref.shape[1]
    tm, sm, tz, sz, w = (every_ref[:, k, :] for k in range(5))
    t_top = jnp.max(tm, axis=0, keepdims=True)
    s_top = jnp.max(sm, axis=0, keepdims=True)
    t_gap, s_gap = tm - t_top, sm - s_top
    t_scale = jnp.exp(t_gap)
    t_total = jnp.sum(tz * t_scale, axis=0, keepdims=True)
    s_total = jnp.sum(sz * jnp.exp(s_gap), axis=0, keepdims=True)
    w_total = jnp.sum(t_scale * (w + tz * (t_gap - s_gap)), axis=0, keepdims=True)
    t_log, s_log = jnp.log(t_total), jnp.log(s_total)
    mismatch = (SOFTENING_HEAT * SOFTENING_HEAT) * (w_total / t_total - t_log + s_log)
    mismatch_ref[...] = mismatch[:, :rows]
    mask_tile[...] = jnp.zeros(mask_tile.shape, jnp.float32)
    mask_tile[0:1, :rows] = mask_ref[...].astype(jnp.float32)
    importance = mask_tile[0:1, :]
    loss = jnp.sum(importance * mismatch, axis=1, keepdims=True)
    count = jnp.sum(importance, axis=1, keepdims=True)
    lane = lax.broadcasted_iota(jnp.int32, (1, LANES), 1)
    sums = jnp.where(lane == 0, loss, jnp.where(lane == 1, count, 0.0))
    sums_ref[...] = jnp.broadcast_to(sums[None], sums_ref.shape)
    row = lax.broadcasted_iota(jnp.int32, (LANES, LANES), 0)
    table = jnp.where(row == 0, t_top + t_log, jnp.where(row == 1, s_top + s_log, importance))
    consts_ref[...] = table.T[:rows]


def gap_kernel(student_ref, a_ref, b_ref, consts_ref, gap_ref):
    width = a_ref.shape[1]
    t_log, s_log = consts_ref[:, 0:1], consts_ref[:, 1:2]
    for k, ref in ((0, a_ref), (1, b_ref)):
        cols = slice(k * width, (k + 1) * width)
        gap_ref[:, cols] = jnp.exp(student_ref[:, cols] - s_log) - jnp.exp(ref[...] - t_log)


def grad_kernel(factor, core_ref, zh_ref, gap_ref, other_ref, sums_ref, consts_ref, grad_ref, loss_ref):
    half = gap_ref.shape[1]
    width = half // 2
    total = jnp.sum(sums_ref[...], axis=0)
    lane = lax.broadcasted_iota(jnp.int32, total.shape, 1)
    loss = jnp.sum(jnp.where(lane == 0, total, 0.0), axis=1, keepdims=True)
    count = jnp.sum(jnp.where(lane == 1, total, 0.0), axis=1, keepdims=True)
    loss_ref[...] = loss / count
    multiplier = consts_ref[:, 2:3] * (factor / count)
    core, zh = core_ref[0], zh_ref[0]
    for ref, c in ((gap_ref, core), (other_ref, 1 - core)):
        for k, at in ((0, zh), (1, 1 - zh)):
            cols = pl.ds(pl.multiple_of(c * half + at * width, LANES), width)
            grad_ref[:, cols] = ref[:, k * width : (k + 1) * width] * multiplier


def local(
    mentor_final_states,
    mentor_output_matrix,
    learner_final_states,
    learner_output_matrix,
    loss_mask,
):
    tokens = mentor_final_states.shape[0]
    width = mentor_output_matrix.shape[1]
    columns = learner_output_matrix.shape[1]
    half = columns // 2
    lexicon = width * lax.axis_size(GROUP)
    rows = lax.axis_size(DP)
    peers = lax.axis_size(("co", "zl"))
    core = lax.axis_index("co")
    zh = lax.axis_index("zh")
    core_at, zh_at = core[None].astype(jnp.int32), zh[None].astype(jnp.int32)
    f32 = jnp.float32

    def product(c):
        matrix = lax.dynamic_slice_in_dim(learner_output_matrix, c * half, half, 1)
        return jnp.dot(learner_final_states, matrix, preferred_element_type=f32)

    give = product(1 - core)
    from_core = lax.ppermute(give, "co", SWAP)
    keep = lax.optimization_barrier(product(core))
    chip_sum = keep + from_core
    other_sum = lax.ppermute(chip_sum, "zh", SWAP)

    block = jnp.dot(mentor_final_states, mentor_output_matrix, preferred_element_type=f32) / SOFTENING_HEAT
    block_a = lax.ppermute(block, GROUP, teacher_route(0))
    block_b = lax.ppermute(block, GROUP, teacher_route(1))

    stats, student = call(
        stats_kernel,
        [jax.ShapeDtypeStruct((peers, SUBLANES, LANES), f32), jax.ShapeDtypeStruct((tokens, half), f32)],
        [VMEM, VMEM],
        [SMEM, VMEM, VMEM, VMEM, VMEM],
    )(zh_at, chip_sum, other_sum, block_a, block_b)
    every = lax.all_to_all(stats, ("zl", "co"), 0, 0)
    mismatch, sums, consts = pl.pallas_call(
        merge_kernel,
        out_shape=[
            jax.ShapeDtypeStruct((1, tokens), f32),
            jax.ShapeDtypeStruct((rows, 1, LANES), f32),
            jax.ShapeDtypeStruct((tokens, LANES), f32),
        ],
        in_specs=[pl.BlockSpec(memory_space=VMEM)] * 2,
        out_specs=[pl.BlockSpec(memory_space=VMEM)] * 3,
        scratch_shapes=[pltpu.VMEM((SUBLANES, LANES), f32)],
        name="merge",
        compiler_params=pltpu.CompilerParams(vmem_limit_bytes=KERNEL_VMEM),
    )(every, loss_mask[None])
    all_sums = lax.all_to_all(sums, DP, 0, 0, axis_index_groups=[SERVED])

    (gap,) = call(
        gap_kernel, [jax.ShapeDtypeStruct((tokens, half), f32)], [VMEM], [VMEM] * 4
    )(student, block_a, block_b, consts)
    other = lax.ppermute(gap, "co", SWAP)

    def final(*refs):
        grad_kernel(SOFTENING_HEAT * lexicon * tokens * rows, *refs)

    student_grad, mean_loss = call(
        final,
        [jax.ShapeDtypeStruct((tokens, columns), f32), jax.ShapeDtypeStruct((1, 1), f32)],
        [VMEM, VMEM],
        [SMEM, SMEM, VMEM, VMEM, VMEM, VMEM],
    )(core_at, zh_at, gap, other, all_sums, consts)
    return mismatch.reshape(tokens), mean_loss.reshape(()), student_grad


def solution(mesh):
    split = Mesh(
        mesh.devices.reshape(mesh.shape["dp"], 2, mesh.shape["mx"] // 2, mesh.shape["my"]),
        ("dp", "zh", "co", "zl"),
    )
    mx = ("zh", "co")
    in_specs = (P(DP, None), P(None, ("zh", "co", "zl")), P(DP, mx), P(mx, "zl"), P(DP))
    out_specs = (P(DP), P(), P(DP, "zl"))

    return jax.shard_map(local, mesh=split, in_specs=in_specs, out_specs=out_specs, check_vma=False)
```
